32 devices in a mesh: data: 4 (over y, z), tensor: 8 (over x, core).
Axes of the slice: x: 4, y: 2, z: 2, core: 2. Of those that a mesh axis runs over, the one named last changes fastest.
The devices are a block of a 4x4x8 slice.
Arguments:
- x_in: bfloat16 [64, 128, 3072], P('data'), parts along dimension 0
- adapter_ids: int32 [64], P('data'), parts along dimension 0
- gain_attn: float32 [3072], replicated
- gain_mlp: float32 [3072], replicated
- w_q: bfloat16 [3072, 16, 256], P(None, 'tensor')
- w_k: bfloat16 [3072, 16, 256], P(None, 'tensor')
- w_v: bfloat16 [3072, 16, 256], P(None, 'tensor')
- w_o: bfloat16 [16, 256, 3072], P('tensor')
- w_gate: bfloat16 [3072, 24576], P(None, 'tensor')
- w_up: bfloat16 [3072, 24576], P(None, 'tensor')
- w_down: bfloat16 [24576, 3072], P('tensor')
- a_q: bfloat16 [8, 3072, 256], P(None, None, 'tensor')
- b_q: bfloat16 [8, 256, 16, 256], P(None, None, 'tensor')
- a_k: bfloat16 [8, 3072, 256], P(None, None, 'tensor')
- b_k: bfloat16 [8, 256, 16, 256], P(None, None, 'tensor')
- a_v: bfloat16 [8, 3072, 256], P(None, None, 'tensor')
- b_v: bfloat16 [8, 256, 16, 256], P(None, None, 'tensor')
- a_o: bfloat16 [8, 16, 256, 256], P(None, 'tensor')
- b_o: bfloat16 [8, 256, 3072], P(None, None, 'tensor')
- a_gate: bfloat16 [8, 3072, 256], P(None, None, 'tensor')
- b_gate: bfloat16 [8, 256, 24576], P(None, None, 'tensor')
- a_up: bfloat16 [8, 3072, 256], P(None, None, 'tensor')
- b_up: bfloat16 [8, 256, 24576], P(None, None, 'tensor')
- a_down: bfloat16 [8, 24576, 256], P(None, 'tensor')
- b_down: bfloat16 [8, 256, 3072], P(None, None, 'tensor')
Outputs:
- output: bfloat16 [64, 128, 3072], P('data'), parts along dimension 0
There are 4 independent parts. The reference program is written for one: setup_inputs(seed, part) draws one part's arguments, and reference() takes and returns one part's arrays. A program takes and returns all parts, laid end to end along the dimension named above; an argument that names none is the same for every part.
All inputs are finite; a program needn't handle non-finite values.
Results may differ from the reference program's by a relative error of at most 0.02.
Values are sent between devices in bfloat16 or wider.
A program may use at most 768 MiB of HBM per device.

```python
import jax
import jax.numpy as jnp
from jax import lax

MODEL_DIM = 3072
FFN_DIM = 24576
NUM_HEADS = 16
KV_HEADS = 16
HEAD_DIM = 256
BATCH = 16
SEQ_LEN = 128
RANK = 256
ADAPTERS = 8
ALPHA = 16
ROPE_BASE = 10000

Q_WIDTH = NUM_HEADS * HEAD_DIM
KV_WIDTH = KV_HEADS * HEAD_DIM
GROUP_SIZE = NUM_HEADS // KV_HEADS
LORA_SCALE = ALPHA / RANK
EPSILON = 1e-5


def draw_ids(key_in):
    key_first, key_second, key_perm = jax.random.split(key_in, 3)
    first_draw = jax.random.randint(key_first, (BATCH,), 0, ADAPTERS)
    second_draw = jax.random.randint(key_second, (BATCH,), 0, ADAPTERS)
    slot_index = jnp.arange(BATCH)
    chosen = jnp.where(slot_index < ADAPTERS, slot_index, jnp.minimum(first_draw, second_draw))
    return jax.random.permutation(key_perm, chosen).astype(jnp.int32)


def setup_inputs(seed: int = 0, part: int = 0) -> dict:
    root_key = jax.random.key(seed)
    key_x, key_ids = jax.random.split(jax.random.fold_in(root_key, part), 2)
    key_list = jax.random.split(root_key, 23)
    b_scale = 0.2 * RANK ** 0.5 / ALPHA

    def normal_bf16(key_in, arr_shape, scale_val):
        return (jax.random.normal(key_in, arr_shape, jnp.float32) * scale_val).astype(jnp.bfloat16)

    return {
        'x_in': normal_bf16(key_x, (BATCH, SEQ_LEN, MODEL_DIM), 1.0),
        'adapter_ids': draw_ids(key_ids),
        'gain_attn': 1.0 + 0.25 * jax.random.normal(key_list[0], (MODEL_DIM,), jnp.float32),
        'gain_mlp': 1.0 + 0.25 * jax.random.normal(key_list[1], (MODEL_DIM,), jnp.float32),
        'w_q': normal_bf16(key_list[2], (MODEL_DIM, NUM_HEADS, HEAD_DIM), 1.6 * MODEL_DIM ** -0.5),
        'w_k': normal_bf16(key_list[3], (MODEL_DIM, KV_HEADS, HEAD_DIM), 1.6 * MODEL_DIM ** -0.5),
        'w_v': normal_bf16(key_list[4], (MODEL_DIM, KV_HEADS, HEAD_DIM), MODEL_DIM ** -0.5),
        'w_o': normal_bf16(key_list[5], (NUM_HEADS, HEAD_DIM, MODEL_DIM), 1.4 * Q_WIDTH ** -0.5),
        'w_gate': normal_bf16(key_list[6], (MODEL_DIM, FFN_DIM), MODEL_DIM ** -0.5),
        'w_up': normal_bf16(key_list[7], (MODEL_DIM, FFN_DIM), MODEL_DIM ** -0.5),
        'w_down': normal_bf16(key_list[8], (FFN_DIM, MODEL_DIM), 1.4 * FFN_DIM ** -0.5),
        'a_q': normal_bf16(key_list[9], (ADAPTERS, MODEL_DIM, RANK), MODEL_DIM ** -0.5),
        'b_q': normal_bf16(key_list[10], (ADAPTERS, RANK, NUM_HEADS, HEAD_DIM), 1.6 * b_scale),
        'a_k': normal_bf16(key_list[11], (ADAPTERS, MODEL_DIM, RANK), MODEL_DIM ** -0.5),
        'b_k': normal_bf16(key_list[12], (ADAPTERS, RANK, KV_HEADS, HEAD_DIM), 1.6 * b_scale),
        'a_v': normal_bf16(key_list[13], (ADAPTERS, MODEL_DIM, RANK), MODEL_DIM ** -0.5),
        'b_v': normal_bf16(key_list[14], (ADAPTERS, RANK, KV_HEADS, HEAD_DIM), b_scale),
        'a_o': normal_bf16(key_list[15], (ADAPTERS, NUM_HEADS, HEAD_DIM, RANK), Q_WIDTH ** -0.5),
        'b_o': normal_bf16(key_list[16], (ADAPTERS, RANK, MODEL_DIM), 1.4 * b_scale),
        'a_gate': normal_bf16(key_list[17], (ADAPTERS, MODEL_DIM, RANK), MODEL_DIM ** -0.5),
        'b_gate': normal_bf16(key_list[18], (ADAPTERS, RANK, FFN_DIM), b_scale),
        'a_up': normal_bf16(key_list[19], (ADAPTERS, MODEL_DIM, RANK), MODEL_DIM ** -0.5),
        'b_up': normal_bf16(key_list[20], (ADAPTERS, RANK, FFN_DIM), b_scale),
        'a_down': normal_bf16(key_list[21], (ADAPTERS, FFN_DIM, RANK), FFN_DIM ** -0.5),
        'b_down': normal_bf16(key_list[22], (ADAPTERS, RANK, MODEL_DIM), 1.4 * b_scale),
    }


def rms_gain(act_in, gain_vec):
    act_f32 = act_in.astype(jnp.float32)
    inv_rms = lax.rsqrt(jnp.mean(act_f32 * act_f32, axis=-1, keepdims=True) + EPSILON)
    return (act_f32 * inv_rms * gain_vec).astype(jnp.bfloat16)


def rope_rotate(head_vals):
    half_dim = HEAD_DIM // 2
    inv_freq = ROPE_BASE ** (-2.0 * jnp.arange(half_dim, dtype=jnp.float32) / HEAD_DIM)
    angle_tab = jnp.arange(SEQ_LEN, dtype=jnp.float32)[:, None] * inv_freq[None, :]
    cos_tab = jnp.cos(angle_tab)[:, None, :]
    sin_tab = jnp.sin(angle_tab)[:, None, :]
    first_half = head_vals[..., :half_dim]
    second_half = head_vals[..., half_dim:]
    return jnp.concatenate([first_half * cos_tab - second_half * sin_tab, second_half * cos_tab + first_half * sin_tab], axis=-1)


def reference(x_in, adapter_ids, gain_attn, gain_mlp, w_q, w_k, w_v, w_o, w_gate, w_up, w_down, a_q, b_q, a_k, b_k, a_v, b_v, a_o, b_o, a_gate, b_gate, a_up, b_up, a_down, b_down):
    flat_q = w_q.reshape(MODEL_DIM, Q_WIDTH)
    flat_k = w_k.reshape(MODEL_DIM, KV_WIDTH)
    flat_v = w_v.reshape(MODEL_DIM, KV_WIDTH)
    flat_o = w_o.reshape(Q_WIDTH, MODEL_DIM)
    causal = jnp.arange(SEQ_LEN)[:, None] >= jnp.arange(SEQ_LEN)[None, :]

    def project(act_in, weight, a_mat, b_mat):
        base_out = jnp.dot(act_in, weight, preferred_element_type=jnp.float32)
        low_rank = jnp.dot(act_in, a_mat, preferred_element_type=jnp.float32).astype(jnp.bfloat16)
        return base_out + LORA_SCALE * jnp.dot(low_rank, b_mat, preferred_element_type=jnp.float32)

    def one_sequence(seq_pair):
        x_seq, adapter = seq_pair
        h_attn = rms_gain(x_seq, gain_attn)
        z_q = project(h_attn, flat_q, a_q[adapter], b_q[adapter].reshape(RANK, Q_WIDTH))
        z_k = project(h_attn, flat_k, a_k[adapter], b_k[adapter].reshape(RANK, KV_WIDTH))
        z_v = project(h_attn, flat_v, a_v[adapter], b_v[adapter].reshape(RANK, KV_WIDTH))
        q_heads = rope_rotate(z_q.reshape(SEQ_LEN, NUM_HEADS, HEAD_DIM)).astype(jnp.bfloat16)
        k_heads = rope_rotate(z_k.reshape(SEQ_LEN, KV_HEADS, HEAD_DIM)).astype(jnp.bfloat16)
        v_heads = z_v.reshape(SEQ_LEN, KV_HEADS, HEAD_DIM).astype(jnp.bfloat16)
        q_group = q_heads.reshape(SEQ_LEN, KV_HEADS, GROUP_SIZE, HEAD_DIM)
        scores = jnp.einsum('skgd,tkd->kgst', q_group.astype(jnp.float32), k_heads.astype(jnp.float32)) * HEAD_DIM ** -0.5
        attn_prob = jax.nn.softmax(jnp.where(causal, scores, -1e30), axis=-1).astype(jnp.bfloat16)
        mixed_out = jnp.einsum('kgst,tkd->skgd', attn_prob.astype(jnp.float32), v_heads.astype(jnp.float32))
        attn_out = mixed_out.astype(jnp.bfloat16).reshape(SEQ_LEN, Q_WIDTH)
        z_o = project(attn_out, flat_o, a_o[adapter].reshape(Q_WIDTH, RANK), b_o[adapter])
        x_mid = (x_seq.astype(jnp.float32) + z_o).astype(jnp.bfloat16)
        h_mlp = rms_gain(x_mid, gain_mlp)
        z_gate = project(h_mlp, w_gate, a_gate[adapter], b_gate[adapter])
        z_up = project(h_mlp, w_up, a_up[adapter], b_up[adapter])
        hidden = (jax.nn.silu(z_gate) * z_up).astype(jnp.bfloat16)
        z_down = project(hidden, w_down, a_down[adapter], b_down[adapter])
        return (x_mid.astype(jnp.float32) + z_down).astype(jnp.bfloat16)

    return lax.map(one_sequence, (x_in, adapter_ids))
```

```python
import functools

import jax
import jax.numpy as jnp
from jax import lax
from jax.experimental import pallas as pl
from jax.experimental.pallas import tpu as pltpu
from jax.sharding import PartitionSpec as P

ALPHA = 16.0
ROPE_BASE = 10000.0
EPSILON = 1e-5
F32 = jnp.float32
BF16 = jnp.bfloat16
MESH = pl.DeviceIdType.MESH
ANY = pl.BlockSpec(memory_space=pl.ANY)
NT = (((1,), (1,)), ((), ()))

SEQS = 4
TILE_N = 256
TILE_D = 512


def dot(a, b, dims=None):
    if dims is None:
        return jnp.dot(a, b, preferred_element_type=F32)
    return lax.dot_general(a, b, dims, preferred_element_type=F32)


def rank_kernel(ids_ref, x_ref, gain_ref, aq_ref, ak_ref, av_ref, h_ref, low_ref):
    x = x_ref[0].astype(F32)
    inv = lax.rsqrt(jnp.mean(x * x, axis=-1, keepdims=True) + EPSILON)
    h = (x * inv * gain_ref[...]).astype(BF16)
    h_ref[...] = h
    a = jnp.concatenate([aq_ref[0], ak_ref[0], av_ref[0]], axis=0)
    low_ref[...] = dot(a, h, NT).astype(BF16)


def rank_products(ids, x, gain, aq, ak, av):
    batch, seq, dim = x.shape
    rank = aq.shape[1]
    a_spec = pl.BlockSpec((1, rank, dim), lambda b, ids: (ids[b], 0, 0))
    return pl.pallas_call(
        rank_kernel,
        grid_spec=pltpu.PrefetchScalarGridSpec(
            num_scalar_prefetch=1,
            grid=(batch,),
            in_specs=[
                pl.BlockSpec((1, seq, dim), lambda b, ids: (b, 0, 0)),
                pl.BlockSpec((1, dim), lambda b, ids: (0, 0)),
                a_spec, a_spec, a_spec,
            ],
            out_specs=[
                pl.BlockSpec((seq, dim), lambda b, ids: (b, 0)),
                pl.BlockSpec((3 * rank, seq), lambda b, ids: (0, b)),
            ],
        ),
        out_shape=[
            jax.ShapeDtypeStruct((batch * seq, dim), BF16),
            jax.ShapeDtypeStruct((3 * rank, batch * seq), BF16),
        ],
        compiler_params=pltpu.CompilerParams(vmem_limit_bytes=40 * 2**20),
        cost_estimate=pl.CostEstimate(flops=2 * batch * seq * dim * 256, bytes_accessed=4 * batch * seq * dim, transcendentals=0),
        name="rank_products",
    )(ids, x, gain, aq, ak, av)


def attention_kernel(scale, ids_ref, h_ref, low_ref, wq_ref, wk_ref, wv_ref, bq_ref, bk_ref, bv_ref, wo_ref, ao_ref,
                     cos_ref, sin_ref, part_ref, lowo_ref, z_ref, lowp_ref, attn_ref):
    c = pl.program_id(0)
    n_dev = low_ref.shape[0]
    rank = low_ref.shape[1] // 3
    tokens = h_ref.shape[0]
    seq = tokens // SEQS
    head = 2 * cos_ref.shape[1]
    heads = wq_ref.shape[1] // head
    half = head // 2
    h = h_ref[...]
    for p, w_ref in enumerate((wq_ref, wk_ref, wv_ref)):
        z_ref[p] = dot(h, w_ref[...])
        cat = jnp.concatenate([low_ref[d, rank * p:rank * (p + 1), :] for d in range(n_dev)], axis=0)
        lowp_ref[p] = jnp.transpose(cat.astype(F32)).astype(BF16)
    rows_i = lax.broadcasted_iota(jnp.int32, (seq, seq), 0)
    cols_i = lax.broadcasted_iota(jnp.int32, (seq, seq), 1)
    causal = rows_i >= cols_i
    cos = cos_ref[...]
    sin = sin_ref[...]

    def one_seq(s, carry):
        rows = pl.ds(pl.multiple_of(s * seq, seq), seq)
        ident = ids_ref[c * SEQS + s]
        zs = []
        for p, b_ref in enumerate((bq_ref, bk_ref, bv_ref)):
            zs.append(z_ref[p, rows, :] + scale * dot(lowp_ref[p, rows, :], b_ref[ident]))
        for hd in range(heads):
            lo = hd * head

            def rope(z):
                a = z[:, lo:lo + half]
                b = z[:, lo + half:lo + head]
                return jnp.concatenate([a * cos - b * sin, b * cos + a * sin], axis=-1).astype(BF16)

            q = rope(zs[0])
            k = rope(zs[1])
            v = zs[2][:, lo:lo + head].astype(BF16)
            sc = dot(q, k, NT) * (head ** -0.5)
            sc = jnp.where(causal, sc, -1e30)
            e = jnp.exp(sc - jnp.max(sc, axis=-1, keepdims=True))
            pr = (e / jnp.sum(e, axis=-1, keepdims=True)).astype(BF16)
            attn_ref[rows, lo:lo + head] = dot(pr, v).astype(BF16)
        lowo_ref[0, rows, :] = dot(attn_ref[rows, :], ao_ref[ident]).astype(BF16)
        return carry

    lax.fori_loop(0, SEQS, one_seq, 0)
    n_chip = part_ref.shape[2]
    bc = part_ref.shape[4]
    for i in range(n_chip):
        val = dot(attn_ref[...], wo_ref[:, 2 * bc * i:2 * bc * (i + 1)]).astype(BF16)
        part_ref[0, 0, i] = val[:, :bc]
        part_ref[0, 1, i] = val[:, bc:]


def attention_stage(ids, h, low, wq, wk, wv, bq, bk, bv, wo, ao, cos, sin, scale):
    total, dim = h.shape
    tokens = cos.shape[0] * SEQS
    chunks = total // tokens
    n_dev = low.shape[0]
    rank = bq.shape[1]
    bc = dim // n_dev
    n_chip = n_dev // 2
    width = wq.shape[1]

    def whole(a):
        nd = a.ndim
        return pl.BlockSpec(a.shape, lambda c, ids: (0,) * nd, pipeline_mode=pl.Buffered(1))

    return pl.pallas_call(
        functools.partial(attention_kernel, scale),
        grid_spec=pltpu.PrefetchScalarGridSpec(
            num_scalar_prefetch=1,
            grid=(chunks,),
            in_specs=[
                pl.BlockSpec((tokens, dim), lambda c, ids: (c, 0)),
                pl.BlockSpec((n_dev, low.shape[1], tokens), lambda c, ids: (0, 0, c)),
                whole(wq), whole(wk), whole(wv), whole(bq), whole(bk), whole(bv), whole(wo), whole(ao), whole(cos), whole(sin),
            ],
            out_specs=[
                pl.BlockSpec((1, 2, n_chip, tokens, bc), lambda c, ids: (c, 0, 0, 0, 0)),
                pl.BlockSpec((1, tokens, rank), lambda c, ids: (c, 0, 0)),
            ],
            scratch_shapes=[
                pltpu.VMEM((3, tokens, width), F32),
                pltpu.VMEM((3, tokens, rank), BF16),
                pltpu.VMEM((tokens, width), BF16),
            ],
        ),
        out_shape=[
            jax.ShapeDtypeStruct((chunks, 2, n_chip, tokens, bc), BF16),
            jax.ShapeDtypeStruct((chunks, tokens, rank), BF16),
        ],
        compiler_params=pltpu.CompilerParams(vmem_limit_bytes=60 * 2**20),
        cost_estimate=pl.CostEstimate(flops=2 * total * dim * width * 4, bytes_accessed=6 * total * dim, transcendentals=0),
        name="attention_stage",
    )(ids, h, low, wq, wk, wv, bq, bk, bv, wo, ao, cos, sin)


def remote(src, dst, ssem, rsem, dev):
    return pltpu.make_async_remote_copy(src_ref=src, dst_ref=dst, send_sem=ssem, recv_sem=rsem,
                                        device_id={"tensor": dev}, device_id_type=MESH)


class Exchange:
    def __init__(self, place, d2d, q, ra, rb, ol, orr, gat, rs_send, rs_recv, ag_send, ag_recv):
        self.k, self.i, self.n, self.left, self.right, self.partner = place
        self.d2d, self.q, self.ra, self.rb, self.ol, self.orr, self.g = d2d, q, ra, rb, ol, orr, gat
        self.ss, self.sr, self.gs, self.gr = rs_send, rs_recv, ag_send, ag_recv
        rows = gat.shape[2]
        self.rows = rows
        self.a = pl.ds(0, rows // 2)
        self.b = pl.ds(rows // 2, rows // 2)

    def chip(self, off):
        return lax.rem(self.i + off + self.n, self.n)

    def rs_copy(self, t, src=None):
        q, a, b = self.q, self.a, self.b
        up, far, down = self.chip(1), self.chip(2), self.chip(-1)
        if t == 0:
            pair = (src if src is not None else self.d2d, self.d2d, self.partner)
        elif t == 1:
            pair = (q.at[far, a], self.ra, self.right)
        elif t == 2:
            pair = (q.at[up, b], self.ol.at[b], self.right)
        elif t == 3:
            pair = (q.at[far, b], self.rb, self.left)
        elif t == 4:
            pair = (q.at[down, a], self.orr.at[a], self.left)
        elif t == 5:
            pair = (q.at[up, a], self.ol.at[a], self.right)
        else:
            pair = (q.at[down, b], self.orr.at[b], self.left)
        return remote(pair[0], pair[1], self.ss.at[t], self.sr.at[t], pair[2])

    def add(self, dst, terms):
        rows = dst.shape[0]
        slab = min(rows, 64)

        def body(s, carry):
            r = pl.ds(pl.multiple_of(s * slab, slab), slab)
            tot = terms[0][r, :].astype(F32)
            for t in terms[1:]:
                tot = tot + t[r, :].astype(F32)
            dst[r, :] = tot.astype(BF16)
            return carry

        lax.fori_loop(0, rows // slab, body, 0)

    def start_rs(self, own):
        self.rs_copy(0).wait_recv()
        for off, sends in ((2, (1, 3)), (1, (2,)), (-1, (4,)), (0, ())):
            j = self.chip(off)
            self.add(self.q.at[j], (own.at[j], self.d2d.at[j]))
            for t in sends:
                self.rs_copy(t).start()

    def relay_rs(self):
        self.rs_copy(1).wait_recv()
        up = self.q.at[self.chip(1), self.a]
        self.rs_copy(3).wait_recv()
        down = self.q.at[self.chip(-1), self.b]
        self.add(up, (up, self.ra))
        self.rs_copy(5).start()
        self.add(down, (down, self.rb))
        self.rs_copy(6).start()

    def wait_rs(self):
        for t in (2, 4, 5, 6):
            self.rs_copy(t).wait_recv()

    def ag_copy(self, t):
        g, k, i = self.g, self.k, self.i
        up, far, down = self.chip(1), self.chip(2), self.chip(-1)
        src, dev = (
            (g.at[k, i], self.right),
            (g.at[k, i], self.left),
            (g.at[k, i], self.partner),
            (g.at[k, down, self.a], self.right),
            (g.at[k, up, self.b], self.left),
            (g.at[k, down], self.partner),
            (g.at[k, up], self.partner),
            (g.at[k, far], self.partner),
        )[t]
        return remote(src, src, self.gs.at[t], self.gr.at[t], dev)

    def ag_wait(self, t):
        g, k, i = self.g, self.k, self.i
        up, far, down = self.chip(1), self.chip(2), self.chip(-1)
        o = 1 - k
        dst = (
            g.at[k, down],
            g.at[k, up],
            g.at[o, i],
            g.at[k, far, self.a],
            g.at[k, far, self.b],
            g.at[o, down],
            g.at[o, up],
            g.at[o, far],
        )[t]
        remote(dst, dst, self.gs.at[t], self.gr.at[t], self.partner).wait_recv()

    def start_ag(self):
        for t in (0, 1, 2):
            self.ag_copy(t).start()

    def relay_ag(self):
        self.ag_wait(0)
        self.ag_copy(3).start()
        self.ag_wait(1)
        self.ag_copy(4).start()
        self.ag_copy(5).start()
        self.ag_copy(6).start()

    def last_ag(self):
        self.ag_wait(3)
        self.ag_wait(4)
        self.ag_copy(7).start()

    def end_ag(self):
        for t in (2, 5, 6, 7):
            self.ag_wait(t)
        for t in range(8):
            self.ag_copy(t).wait_send()

    def end_rs(self):
        for t in range(1, 7):
            self.rs_copy(t).wait_send()


R1_TICKS = (0, 1, 4, 5, 6, 7, 8, 10, 12, 13, 14, 15, 17)
R2_TICKS = (0, 2, 6, 7, 8, 9, 11, 14, 16, 17)


def mlp_kernel(scale, n_dev, ids_ref, part_hbm, lowo_hbm, x_hbm, bo_hbm, bd_hbm, agu_hbm, gain_ref,
               wg_ref, wu_ref, bg_ref, bu_ref, ad_ref, wd_ref, y_hbm,
               h2, lowg, lowu, m_ref, lowd, x1own, xres, bo, bd, agu,
               q1, d1, ra1, rb1, ol1, or1, g1, lq1, ld1, lra1, lrb1, lol1, lor1, lg1, gu,
               part2, q2, d2, ra2, rb2, ol2, or2, g2, lpart2, lq2, ld2, lra2, lrb2, lol2, lor2, lg2,
               load_sem, own_sem, y_sem, s_sem, r_sem):
    w = pl.program_id(0)
    j = pl.program_id(1)
    me = lax.axis_index("tensor")
    n = n_dev // 2
    i = me // 2
    k = lax.rem(me, 2)
    right = lax.rem(me + 2, n_dev)
    left = lax.rem(me + n_dev - 2, n_dev)
    partner = me + 1 - 2 * k
    place = (k, i, n, left, right, partner)
    chunks, _, _, tokens, bc = part_hbm.shape
    seq = tokens // SEQS
    gate_ticks = m_ref.shape[1] // TILE_N
    dim = h2.shape[2]

    def sems(t):
        return s_sem.at[t, 0], r_sem.at[t, 0], s_sem.at[t, 1], r_sem.at[t, 1]

    e1 = Exchange(place, d1, q1, ra1, rb1, ol1, or1, g1, *sems(0))
    f1 = Exchange(place, ld1, lq1, lra1, lrb1, lol1, lor1, lg1, *sems(1))
    e2 = Exchange(place, d2, q2, ra2, rb2, ol2, or2, g2, *sems(2))
    f2 = Exchange(place, ld2, lq2, lra2, lrb2, lol2, lor2, lg2, *sems(3))
    eg = Exchange(place, None, None, None, None, None, None, gu, *sems(4))

    def loads():
        return [pltpu.make_async_copy(src, dst, load_sem.at[t])
                for t, (src, dst) in enumerate(((bo_hbm, bo), (agu_hbm, agu), (bd_hbm, bd)))]

    def rows_of(s):
        return pl.ds(s * seq, seq)

    def low_rows(ref, s):
        rows = ref.shape[2]
        per = seq // rows
        return jnp.concatenate([ref[b // n, b % n] for b in range(s * per, (s + 1) * per)], axis=0)

    @pl.when((w == 0) & (j == 0))
    def _():
        barrier = pltpu.get_barrier_semaphore()
        for dev in (left, right, partner):
            pl.semaphore_signal(barrier, inc=1, device_id={"tensor": dev}, device_id_type=MESH)
        for cp in loads():
            cp.start()
        pl.semaphore_wait(barrier, 3)

    def own_loads():
        return (
            pltpu.make_async_copy(part_hbm.at[w, k], q1, own_sem.at[0]),
            pltpu.make_async_copy(lowo_hbm.at[w, k], lq1, own_sem.at[1]),
            pltpu.make_async_copy(x_hbm.at[pl.ds(w * tokens, tokens), pl.ds(pl.multiple_of(me * bc, bc), bc)], xres, own_sem.at[2]),
        )

    def p1_0():
        f1.rs_copy(0, lowo_hbm.at[w, 1 - k]).start()
        e1.rs_copy(0, part_hbm.at[w, 1 - k]).start()
        for cp in own_loads():
            cp.start()

    def p1_1():
        for cp in own_loads():
            cp.wait()
        f1.start_rs(lq1)
        e1.start_rs(q1)
        f1.rs_copy(0, lowo_hbm.at[w, 1 - k]).wait_send()
        e1.rs_copy(0, part_hbm.at[w, 1 - k]).wait_send()

    def p1_2():
        f1.relay_rs()
        e1.relay_rs()

    def low_sum(f):
        f.wait_rs()
        f.add(f.g.at[f.k, f.i], (f.q.at[f.i], f.ol, f.orr))
        f.start_ag()

    def final_sum(e, f, resid, table, chunk, keep):
        f.end_ag()
        e.wait_rs()
        for s in range(SEQS):
            r = rows_of(s)
            tot = resid[r, :].astype(F32) + (e.q[e.i, r, :].astype(F32) + e.ol[r, :].astype(F32) + e.orr[r, :].astype(F32))
            ident = ids_ref[chunk * SEQS + s]
            tot = tot + scale * dot(low_rows(f.g, s), table[ident])
            val = tot.astype(BF16)
            e.g[e.k, e.i, r, :] = val
            if keep is not None:
                keep[r, :] = val
        e.start_ag()
        e.end_rs()
        f.end_rs()

    def p1_6():
        @pl.when(w == 0)
        def _():
            for cp in loads():
                cp.wait()

        final_sum(e1, f1, xres, bo, w, x1own.at[w])

    def p1_9():
        e1.end_ag()
        slot = lax.rem(w, 2)
        hc = h2.at[slot]
        slab = 32

        def body(t, carry):
            r = pl.ds(pl.multiple_of(t * slab, slab), slab)
            tot = None
            for b in range(n_dev):
                v = g1[b % 2, b // 2, r, :].astype(F32)
                sq = jnp.sum(v * v, axis=-1, keepdims=True)
                tot = sq if tot is None else tot + sq
            inv = lax.rsqrt(tot / dim + EPSILON)
            for b in range(n_dev):
                v = g1[b % 2, b // 2, r, :].astype(F32)
                hc[r, bc * b:bc * (b + 1)] = (v * inv * gain_ref[:, bc * b:bc * (b + 1)]).astype(BF16)
            return carry

        lax.fori_loop(0, tokens // slab, body, 0)
        for s in range(SEQS):
            ident = ids_ref[w * SEQS + s]
            gu[k, i, :, s * seq:(s + 1) * seq] = dot(agu[ident], hc[rows_of(s), :], NT).astype(BF16)
        eg.start_ag()

    def p1_12():
        eg.end_ag()
        slot = lax.rem(w, 2)
        half = gu.shape[2] // 2
        for p, ref in enumerate((lowg, lowu)):
            cat = jnp.concatenate([gu[d % 2, d // 2, half * p:half * (p + 1), :] for d in range(n_dev)], axis=0)
            ref[slot] = jnp.transpose(cat.astype(F32)).astype(BF16)

    steps1 = (p1_0, p1_1, p1_2, lambda: low_sum(f1), f1.relay_ag, f1.last_ag, p1_6, e1.relay_ag, e1.last_ag,
              p1_9, eg.relay_ag, eg.last_ag, p1_12)

    def y_copies():
        rows = pl.ds((w - 2) * tokens, tokens)
        return [pltpu.make_async_copy(g2.at[b % 2, b // 2], y_hbm.at[rows, pl.ds(b * bc, bc)], y_sem.at[b]) for b in range(n_dev)]

    def p2_0():
        f2.rs_copy(0, lpart2.at[1 - k]).start()
        e2.rs_copy(0, part2.at[1 - k]).start()

    def p2_1():
        f2.start_rs(lpart2.at[k])
        e2.start_rs(part2.at[k])
        f2.rs_copy(0, lpart2.at[1 - k]).wait_send()
        e2.rs_copy(0, part2.at[1 - k]).wait_send()

    def p2_2():
        f2.relay_rs()
        e2.relay_rs()

    def p2_6():
        final_sum(e2, f2, x1own.at[w - 2], bd, w - 2, None)

    def p2_9():
        e2.end_ag()
        for cp in y_copies():
            cp.start()
        for cp in y_copies():
            cp.wait()

    steps2 = (p2_0, p2_1, p2_2, lambda: low_sum(f2), f2.relay_ag, f2.last_ag, p2_6, e2.relay_ag, e2.last_ag, p2_9)

    for tick, step in zip(R1_TICKS, steps1):
        pl.when((w < chunks) & (j == tick))(step)
    for tick, step in zip(R2_TICKS, steps2):
        pl.when((w >= 2) & (j == tick))(step)

    live = (w >= 1) & (w <= chunks)

    @pl.when(live & (j == 0))
    def _():
        lowd[...] = jnp.zeros_like(lowd)

    @pl.when(live & (j < gate_ticks))
    def _():
        slot = lax.rem(w + 1, 2)
        g = dot(h2[slot], wg_ref[...])
        u = dot(h2[slot], wu_ref[...])
        cols = pl.ds(pl.multiple_of(j * TILE_N, TILE_N), TILE_N)
        for s in range(SEQS):
            r = rows_of(s)
            ident = ids_ref[(w - 1) * SEQS + s]
            gs = g[s * seq:(s + 1) * seq] + scale * dot(lowg[slot, r, :], bg_ref[ident])
            us = u[s * seq:(s + 1) * seq] + scale * dot(lowu[slot, r, :], bu_ref[ident])
            mm = (jax.nn.silu(gs) * us).astype(BF16)
            m_ref[r, cols] = mm
            lowd[r, :] += dot(mm, ad_ref[ident])

    @pl.when(live & (j == gate_ticks))
    def _():
        rows = lpart2.shape[2]
        for b in range(n_dev):
            lpart2[b // n, b % n] = lowd[b * rows:(b + 1) * rows, :].astype(BF16)

    @pl.when(live & (j >= gate_ticks))
    def _():
        jj = j - gate_ticks
        val = dot(m_ref[...], wd_ref[...]).astype(BF16)
        per = bc // 128
        for t in range(TILE_D // 128):
            unit = jj * (TILE_D // 128) + t
            b = unit // per
            off = pl.multiple_of((unit - b * per) * 128, 128)
            part2[lax.rem(b, 2), b // 2, :, pl.ds(off, 128)] = val[:, t * 128:(t + 1) * 128]


def mlp_stage(ids, part, lowo, x, bo, bd, agu, gain, wg, wu, bg, bu, ad, wd, scale, n_dev):
    chunks, _, n_chip, tokens, bc = part.shape
    total, dim = x.shape
    ffn = wg.shape[1]
    n_ad, rank = bo.shape[0], bo.shape[1]
    lrows = tokens // n_dev
    gur = agu.shape[1]
    gt = ffn // TILE_N
    dt = dim // TILE_D

    def gate_idx(w, j):
        t = jnp.minimum(j, gt - 1)
        return jnp.where(w == 0, 0, jnp.where(w > chunks, gt - 1, t))

    def down_idx(w, j):
        t = jnp.maximum(j - gt, 0)
        return jnp.where(w == 0, 0, jnp.where(w > chunks, dt - 1, t))

    def bufs(rows, cols):
        blk = (n_chip, rows, cols)
        return [
            pltpu.VMEM(blk, BF16), pltpu.VMEM(blk, BF16), pltpu.VMEM((rows // 2, cols), BF16), pltpu.VMEM((rows // 2, cols), BF16),
            pltpu.VMEM((rows, cols), BF16), pltpu.VMEM((rows, cols), BF16), pltpu.VMEM((2,) + blk, BF16),
        ]

    return pl.pallas_call(
        functools.partial(mlp_kernel, scale, n_dev),
        grid=(chunks + 2, gt + dt),
        in_specs=[
            pl.BlockSpec(memory_space=pltpu.SMEM), ANY, ANY, ANY, ANY, ANY, ANY,
            pl.BlockSpec((1, dim), lambda w, j: (0, 0)),
            pl.BlockSpec((dim, TILE_N), lambda w, j: (0, gate_idx(w, j))),
            pl.BlockSpec((dim, TILE_N), lambda w, j: (0, gate_idx(w, j))),
            pl.BlockSpec((n_ad, rank, TILE_N), lambda w, j: (0, 0, gate_idx(w, j))),
            pl.BlockSpec((n_ad, rank, TILE_N), lambda w, j: (0, 0, gate_idx(w, j))),
            pl.BlockSpec((n_ad, TILE_N, rank), lambda w, j: (0, gate_idx(w, j), 0)),
            pl.BlockSpec((ffn, TILE_D), lambda w, j: (0, down_idx(w, j))),
        ],
        out_specs=ANY,
        out_shape=jax.ShapeDtypeStruct((total, dim), BF16),
        scratch_shapes=[
            pltpu.VMEM((2, tokens, dim), BF16),
            pltpu.VMEM((2, tokens, rank), BF16),
            pltpu.VMEM((2, tokens, rank), BF16),
            pltpu.VMEM((tokens, ffn), BF16),
            pltpu.VMEM((tokens, rank), F32),
            pltpu.VMEM((chunks, tokens, bc), BF16),
            pltpu.VMEM((tokens, bc), BF16),
            pltpu.VMEM(bo.shape, BF16),
            pltpu.VMEM(bd.shape, BF16),
            pltpu.VMEM(agu.shape, BF16),
            *bufs(tokens, bc),
            *bufs(lrows, rank),
            pltpu.VMEM((2, n_chip, gur, tokens), BF16),
            pltpu.VMEM((2, n_chip, tokens, bc), BF16),
            *bufs(tokens, bc),
            pltpu.VMEM((2, n_chip, lrows, rank), BF16),
            *bufs(lrows, rank),
            pltpu.SemaphoreType.DMA((3,)),
            pltpu.SemaphoreType.DMA((3,)),
            pltpu.SemaphoreType.DMA((n_dev,)),
            pltpu.SemaphoreType.DMA((5, 2, 8)),
            pltpu.SemaphoreType.DMA((5, 2, 8)),
        ],
        compiler_params=pltpu.CompilerParams(collective_id=0, has_side_effects=True, vmem_limit_bytes=67043328),
        name="mlp_stage",
    )(ids, part, lowo, x, bo, bd, agu, gain, wg, wu, bg, bu, ad, wd)


def solution(mesh):
    tp_size = mesh.shape['tensor']
    head_split = P(None, 'tensor', None)
    last_split = P(None, None, 'tensor')
    b_head_split = P(None, None, 'tensor', None)
    in_specs = (P('data', None, None), P('data'), P(None), P(None),
                head_split, head_split, head_split, P('tensor', None, None),
                P(None, 'tensor'), P(None, 'tensor'), P('tensor', None),
                last_split, b_head_split, last_split, b_head_split, last_split, b_head_split,
                P(None, 'tensor', None, None), last_split,
                last_split, last_split, last_split, last_split,
                P(None, 'tensor', None), last_split)

    def local_layer(x_in, adapter_ids, gain_attn, gain_mlp, w_q, w_k, w_v, w_o, w_gate, w_up, w_down, a_q, b_q, a_k, b_k, a_v, b_v, a_o, b_o, a_gate, b_gate, a_up, b_up, a_down, b_down):
        scale = ALPHA / b_q.shape[1]
        batch, seq, dim = x_in.shape
        head = w_q.shape[2]
        half = head // 2
        n_ad, rank = b_q.shape[:2]

        def flip(a):
            return jnp.swapaxes(a, 1, 2)

        def flat(w):
            return w.reshape(w.shape[:-2] + (w.shape[-2] * w.shape[-1],))

        h, low = rank_products(adapter_ids, x_in, gain_attn[None, :], flip(a_q), flip(a_k), flip(a_v))
        low_all = lax.all_gather(low, 'tensor', axis=0)
        inv_freq = ROPE_BASE ** (-2.0 * jnp.arange(half, dtype=F32) / head)
        angle = jnp.arange(seq, dtype=F32)[:, None] * inv_freq[None, :]
        part, lowo = attention_stage(adapter_ids, h, low_all, flat(w_q), flat(w_k), flat(w_v), flat(b_q), flat(b_k), flat(b_v),
                                     w_o.reshape(-1, dim), a_o.reshape(n_ad, -1, rank), jnp.cos(angle), jnp.sin(angle), scale)
        chunks, tokens = lowo.shape[:2]
        lowo = lowo.reshape(chunks, 2, tp_size // 2, tokens // tp_size, rank)
        agu = jnp.concatenate([flip(a_gate), flip(a_up)], axis=1)
        y = mlp_stage(adapter_ids, part, lowo, x_in.reshape(batch * seq, dim), b_o, b_down, agu, gain_mlp[None, :],
                      w_gate, w_up, b_gate, b_up, a_down, w_down, scale, tp_size)
        return y.reshape(batch, seq, dim)

    return jax.shard_map(local_layer, mesh=mesh, in_specs=in_specs, out_specs=P('data', None, None), check_vma=False)
```

```python
import functools

import jax
import jax.numpy as jnp
from jax import lax
from jax.experimental import pallas as pl
from jax.experimental.pallas import tpu as pltpu
from jax.sharding import PartitionSpec as P

ALPHA = 16.0
ROPE_BASE = 10000.0
EPSILON = 1e-5
F32 = jnp.float32
BF16 = jnp.bfloat16
MESH = pl.DeviceIdType.MESH
ANY = pl.BlockSpec(memory_space=pl.ANY)
NT = (((1,), (1,)), ((), ()))

SEQS = 4
TILE_N = 256
TILE_D = 512


def dot(a, b, dims=None):
    if dims is None:
        return jnp.dot(a, b, preferred_element_type=F32)
    return lax.dot_general(a, b, dims, preferred_element_type=F32)


def rank_kernel(ids_ref, x_ref, gain_ref, aq_ref, ak_ref, av_ref, h_ref, low_ref):
    x = x_ref[0].astype(F32)
    inv = lax.rsqrt(jnp.mean(x * x, axis=-1, keepdims=True) + EPSILON)
    h = (x * inv * gain_ref[...]).astype(BF16)
    h_ref[...] = h
    a = jnp.concatenate([aq_ref[0], ak_ref[0], av_ref[0]])
    low_ref[...] = jnp.transpose(dot(h, a, NT)).astype(BF16)


def rank_products(ids, x, gain, aq, ak, av):
    batch, seq, dim = x.shape
    rank = aq.shape[1]
    a_spec = pl.BlockSpec((1, rank, dim), lambda b, ids: (ids[b], 0, 0))
    return pl.pallas_call(
        rank_kernel,
        grid_spec=pltpu.PrefetchScalarGridSpec(
            num_scalar_prefetch=1,
            grid=(batch,),
            in_specs=[
                pl.BlockSpec((1, seq, dim), lambda b, ids: (b, 0, 0)),
                pl.BlockSpec((1, dim), lambda b, ids: (0, 0)),
                a_spec, a_spec, a_spec,
            ],
            out_specs=[
                pl.BlockSpec((seq, dim), lambda b, ids: (b, 0)),
                pl.BlockSpec((3 * rank, seq), lambda b, ids: (0, b)),
            ],
        ),
        out_shape=[
            jax.ShapeDtypeStruct((batch * seq, dim), BF16),
            jax.ShapeDtypeStruct((3 * rank, batch * seq), BF16),
        ],
        compiler_params=pltpu.CompilerParams(vmem_limit_bytes=60 * 2**20),
        cost_estimate=pl.CostEstimate(flops=2 * batch * seq * dim * 256, bytes_accessed=4 * batch * seq * dim, transcendentals=0),
        name="rank_products",
    )(ids, x, gain, aq, ak, av)


PIECE = 128


class Remote:
    def __init__(self, src, dst, ssem, rsem, dev):
        self.parts = (src, dst, ssem, rsem, dev)

    def make(self, src, dst):
        _, _, ssem, rsem, dev = self.parts
        return pltpu.make_async_remote_copy(src_ref=src, dst_ref=dst, send_sem=ssem, recv_sem=rsem,
                                            device_id={"tensor": dev}, device_id_type=MESH)

    def pieces(self):
        src, dst = self.parts[:2]
        if len(dst.shape) == 3:
            return [self.make(src.at[p], dst.at[p]) for p in range(dst.shape[0])]
        step = min(PIECE if dst.shape[1] <= 512 else 48, dst.shape[0])
        return [self.make(src.at[pl.ds(p, step)], dst.at[pl.ds(p, step)]) for p in range(0, dst.shape[0], step)]

    def start(self):
        start_all(self)

    def wait_send(self):
        self.make(*self.parts[:2]).wait_send()

    def wait_recv(self):
        self.make(*self.parts[:2]).wait_recv()


def start_all(*copies):
    lists = [c.pieces() for c in copies]
    for t in range(max(len(l) for l in lists)):
        for l in lists:
            if t < len(l):
                l[t].start()


def remote(src, dst, ssem, rsem, dev):
    return Remote(src, dst, ssem, rsem, dev)


def placement(n_dev):
    me = lax.axis_index("tensor")
    k = lax.rem(me, 2)
    return k, me // 2, n_dev // 2, lax.rem(me + n_dev - 2, n_dev), lax.rem(me + 2, n_dev), me + 1 - 2 * k


def greet(place):
    barrier = pltpu.get_barrier_semaphore()
    for dev in place[3:]:
        pl.semaphore_signal(barrier, inc=1, device_id={"tensor": dev}, device_id_type=MESH)
    return barrier


class Exchange:
    def __init__(self, place, d2d, q, ra, rb, ol, orr, gat, rs_send, rs_recv, ag_send, ag_recv):
        self.k, self.i, self.n, self.left, self.right, self.partner = place
        self.d2d, self.q, self.ra, self.rb, self.ol, self.orr, self.g = d2d, q, ra, rb, ol, orr, gat
        self.ss, self.sr, self.gs, self.gr = rs_send, rs_recv, ag_send, ag_recv
        rows = gat.shape[2]
        self.rows = rows
        self.a = pl.ds(0, rows // 2)
        self.b = pl.ds(rows // 2, rows // 2)

    def chip(self, off):
        return lax.rem(self.i + off + self.n, self.n)

    def rs_copy(self, t, src=None):
        q, a, b = self.q, self.a, self.b
        up, far, down = self.chip(1), self.chip(2), self.chip(-1)
        if t == 0:
            pair = (src if src is not None else self.d2d, self.d2d, self.partner)
        elif t == 1:
            pair = (q.at[far, a], self.ra, self.right)
        elif t == 2:
            pair = (q.at[up, b], self.ol.at[b], self.right)
        elif t == 3:
            pair = (q.at[far, b], self.rb, self.left)
        elif t == 4:
            pair = (q.at[down, a], self.orr.at[a], self.left)
        elif t == 5:
            pair = (q.at[up, a], self.ol.at[a], self.right)
        else:
            pair = (q.at[down, b], self.orr.at[b], self.left)
        return remote(pair[0], pair[1], self.ss.at[t], self.sr.at[t], pair[2])

    def add(self, dst, terms):
        rows = dst.shape[0]
        slab = min(rows, 64)

        def body(s, carry):
            r = pl.ds(pl.multiple_of(s * slab, slab), slab)
            tot = terms[0][r, :].astype(F32)
            for t in terms[1:]:
                tot = tot + t[r, :].astype(F32)
            dst[r, :] = tot.astype(BF16)
            return carry

        lax.fori_loop(0, rows // slab, body, 0)

    def start_rs(self, own):
        self.rs_copy(0).wait_recv()
        for off, sends in ((2, (1, 3)), (1, (2,)), (-1, (4,)), (0, ())):
            j = self.chip(off)
            self.add(self.q.at[j], (own.at[j], self.d2d.at[j]))
            if sends:
                start_all(*[self.rs_copy(t) for t in sends])

    def relay_rs(self):
        self.rs_copy(1).wait_recv()
        up = self.q.at[self.chip(1), self.a]
        self.rs_copy(3).wait_recv()
        down = self.q.at[self.chip(-1), self.b]
        self.add(up, (up, self.ra))
        self.rs_copy(5).start()
        self.add(down, (down, self.rb))
        self.rs_copy(6).start()

    def wait_rs(self):
        for t in (2, 4, 5, 6):
            self.rs_copy(t).wait_recv()

    def ag_copy(self, t):
        g, k, i = self.g, self.k, self.i
        up, far, down = self.chip(1), self.chip(2), self.chip(-1)
        a, b = self.a, self.b
        src, dev = (
            (g.at[k, i, a], self.right),
            (g.at[k, i, b], self.left),
            (g.at[k, i], self.partner),
            (g.at[k, down, a], self.right),
            (g.at[k, up, b], self.left),
            (g.at[k, down], self.partner),
            (g.at[k, up], self.partner),
            (g.at[k, far], self.partner),
            (g.at[k, i, b], self.right),
            (g.at[k, i, a], self.left),
        )[t]
        return remote(src, src, self.gs.at[t], self.gr.at[t], dev)

    def ag_wait(self, t):
        g, k, i = self.g, self.k, self.i
        up, far, down = self.chip(1), self.chip(2), self.chip(-1)
        o = 1 - k
        dst = (
            g.at[k, down, self.a],
            g.at[k, up, self.b],
            g.at[o, i],
            g.at[k, far, self.a],
            g.at[k, far, self.b],
            g.at[o, down],
            g.at[o, up],
            g.at[o, far],
            g.at[k, down, self.b],
            g.at[k, up, self.a],
        )[t]
        remote(dst, dst, self.gs.at[t], self.gr.at[t], self.partner).wait_recv()

    def start_ag(self):
        start_all(*[self.ag_copy(t) for t in (0, 1)])
        start_all(*[self.ag_copy(t) for t in (8, 9, 2)])

    def relay_ag(self):
        self.ag_wait(0)
        self.ag_copy(3).start()
        self.ag_wait(1)
        self.ag_copy(4).start()

    def last_ag(self):
        self.ag_wait(8)
        self.ag_copy(5).start()
        self.ag_wait(9)
        self.ag_copy(6).start()
        self.ag_wait(3)
        self.ag_wait(4)
        self.ag_copy(7).start()

    def end_ag(self):
        for t in (2, 5, 6, 7):
            self.ag_wait(t)
        for t in range(10):
            self.ag_copy(t).wait_send()

    def end_rs(self):
        for t in range(1, 7):
            self.rs_copy(t).wait_send()


def gather_only(place, gat, send, recv):
    return Exchange(place, *[None] * 6, gat, None, None, send, recv)


def low_sum(f):
    f.wait_rs()
    f.add(f.g.at[f.k, f.i], (f.q.at[f.i], f.ol, f.orr))
    f.start_ag()


def low_rows(ref, s, seq):
    n, rows = ref.shape[1:3]
    per = seq // rows
    return jnp.concatenate([ref[b // n, b % n] for b in range(s * per, (s + 1) * per)])


def total_block(scale, e, f, resid, table, ids_ref, chunk, keep):
    f.end_ag()
    e.wait_rs()
    seq = e.rows // SEQS
    for s in range(SEQS):
        r = pl.ds(s * seq, seq)
        tot = resid[r, :].astype(F32) + (e.q[e.i, r, :].astype(F32) + e.ol[r, :].astype(F32) + e.orr[r, :].astype(F32))
        tot = tot + scale * dot(low_rows(f.g, s, seq), table[ids_ref[chunk * SEQS + s]])
        val = tot.astype(BF16)
        e.g[e.k, e.i, r, :] = val
        if keep is not None:
            keep[r, :] = val
    e.start_ag()
    e.end_rs()
    f.end_rs()


def exchange_bufs(n_chip, rows, cols):
    blk = (n_chip, rows, cols)
    return [
        pltpu.VMEM(blk, BF16), pltpu.VMEM(blk, BF16), pltpu.VMEM((rows // 2, cols), BF16), pltpu.VMEM((rows // 2, cols), BF16),
        pltpu.VMEM((rows, cols), BF16), pltpu.VMEM((rows, cols), BF16), pltpu.VMEM((2,) + blk, BF16),
    ]


def attention_kernel(scale, n_dev, ids_ref, h_ref, low_hbm, x_hbm, wq_ref, wk_ref, wv_ref, bq_ref, bk_ref, bv_ref, wo_ref, ao_ref,
                     bo_ref, cos_ref, sin_ref, part_ref, lowo_ref, g0_hbm, z_ref, lowp_ref, attn_ref, gat, xres,
                     q1, d1, ra1, rb1, ol1, or1, g1, lq1, ld1, lra1, lrb1, lol1, lor1, lg1, load_sem, s_sem, r_sem):
    step = pl.program_id(0)
    chunks = z_ref.shape[0]
    place = placement(n_dev)
    k, i = place[:2]
    pairs = [ref.at[t] for t in range(4) for ref in (s_sem, r_sem)]
    ex = gather_only(place, gat, s_sem.at[4], r_sem.at[4])
    e1 = Exchange(place, d1, q1, ra1, rb1, ol1, or1, g1, *pairs[:4])
    f1 = Exchange(place, ld1, lq1, lra1, lrb1, lol1, lor1, lg1, *pairs[4:])
    tokens, bc = xres.shape
    load_low = pltpu.make_async_copy(low_hbm, gat.at[k, i], load_sem.at[0])
    cols = pl.ds(pl.multiple_of((2 * i + k) * bc, bc), bc)
    load_x = pltpu.make_async_copy(x_hbm.at[pl.ds(0, tokens), cols], xres, load_sem.at[1])

    @pl.when(step == 0)
    def _():
        barrier = greet(place)
        load_low.start()
        load_x.start()
        load_low.wait()
        load_x.wait()
        pl.semaphore_wait(barrier, 3)
        ex.start_ag()

    first = step == chunks - 1
    pl.when(first)(ex.end_ag)

    @pl.when((step < chunks - 1) | (step == chunks))
    def _():
        h = h_ref[...]
        c = jnp.where(step == chunks, chunks - 1, step)
        for p, w_ref in enumerate((wq_ref, wk_ref, wv_ref)):
            z_ref[c, p] = dot(h, w_ref[...])

    pl.when(step == 1)(ex.relay_ag)
    pl.when(step == 2)(ex.last_ag)

    def p1():
        f1.start_rs(lowo_ref.at[0, k])
        e1.start_rs(part_ref.at[0, k])
        f1.rs_copy(0, lowo_ref.at[0, 1 - k]).wait_send()
        e1.rs_copy(0, part_ref.at[0, 1 - k]).wait_send()

    def relays():
        f1.relay_rs()
        e1.relay_rs()

    def finish():
        e1.last_ag()
        e1.end_ag()
        store = pltpu.make_async_copy(g1, g0_hbm, load_sem.at[2])
        store.start()
        store.wait()

    sums = {
        (chunks + 1, 2): relays,
        (chunks + 2, 0): lambda: low_sum(f1),
        (chunks + 2, 1): f1.relay_ag,
        (chunks + 2, 2): f1.last_ag,
        (chunks + 3, 0): lambda: total_block(scale, e1, f1, xres, bo_ref, ids_ref, 0, None),
        (chunks + 3, 2): e1.relay_ag,
        (chunks + 3, 3): finish,
    }

    def slot(t):
        for (when, where), todo in sums.items():
            if where == t:
                pl.when(step == when)(todo)

    @pl.when(first | (step > chunks))
    def _():
        attend(scale, n_dev, jnp.where(first, 0, step - chunks), slot, ids_ref, (bq_ref, bk_ref, bv_ref), wo_ref, ao_ref, cos_ref, sin_ref,
               part_ref, lowo_ref, z_ref, lowp_ref, attn_ref, gat)

    @pl.when(first)
    def _():
        f1.rs_copy(0, lowo_ref.at[0, 1 - k]).start()
        e1.rs_copy(0, part_ref.at[0, 1 - k]).start()

    pl.when(step == chunks)(p1)


def attend(scale, n_dev, c, slot, ids_ref, b_refs, wo_ref, ao_ref, cos_ref, sin_ref, part_ref, lowo_ref, z_ref, lowp_ref, attn_ref, gat):
    rank = gat.shape[2] // 3
    tokens = z_ref.shape[2]
    seq = tokens // SEQS
    head = 2 * cos_ref.shape[1]
    heads = z_ref.shape[3] // head
    half = head // 2
    toks = pl.ds(pl.multiple_of(c * tokens, tokens), tokens)
    for p in range(3):
        cat = jnp.concatenate([gat[d % 2, d // 2, rank * p:rank * (p + 1), toks] for d in range(n_dev)])
        lowp_ref[p] = jnp.transpose(cat.astype(F32)).astype(BF16)
    rows_i = lax.broadcasted_iota(jnp.int32, (seq, seq), 0)
    cols_i = lax.broadcasted_iota(jnp.int32, (seq, seq), 1)
    causal = rows_i >= cols_i
    cos = cos_ref[...]
    sin = sin_ref[...]

    def one_seq(s, carry):
        rows = pl.ds(pl.multiple_of(s * seq, seq), seq)
        ident = ids_ref[c * SEQS + s]
        zs = []
        for p, b_ref in enumerate(b_refs):
            zs.append(z_ref[c, p, rows, :] + scale * dot(lowp_ref[p, rows, :], b_ref[ident]))
        for hd in range(heads):
            lo = hd * head

            def rope(z):
                a = z[:, lo:lo + half]
                b = z[:, lo + half:lo + head]
                return jnp.concatenate([a * cos - b * sin, b * cos + a * sin], axis=-1).astype(BF16)

            q = rope(zs[0])
            k = rope(zs[1])
            v = zs[2][:, lo:lo + head].astype(BF16)
            sc = dot(q, k, NT) * (head ** -0.5)
            sc = jnp.where(causal, sc, -1e30)
            e = jnp.exp(sc - jnp.max(sc, axis=-1, keepdims=True))
            pr = (e / jnp.sum(e, axis=-1, keepdims=True)).astype(BF16)
            attn_ref[rows, lo:lo + head] = dot(pr, v).astype(BF16)
        low = dot(attn_ref[rows, :], ao_ref[ident]).astype(BF16)
        n, per = lowo_ref.shape[2:4]
        for t in range(seq // per):
            b = s * (seq // per) + t
            lowo_ref[0, b // n, lax.rem(b, n)] = low[t * per:(t + 1) * per]
        return carry

    slot(0)
    lax.fori_loop(0, SEQS // 2, one_seq, 0)
    slot(1)
    lax.fori_loop(SEQS // 2, SEQS, one_seq, 0)
    slot(2)
    n_chip = part_ref.shape[2]
    bc = part_ref.shape[4]
    for i in range(n_chip):
        val = dot(attn_ref[...], wo_ref[:, 2 * bc * i:2 * bc * (i + 1)]).astype(BF16)
        part_ref[0, 0, i] = val[:, :bc]
        part_ref[0, 1, i] = val[:, bc:]
    slot(3)


def attention_stage(ids, h, low, x, wq, wk, wv, bq, bk, bv, wo, ao, bo, cos, sin, scale, n_dev):
    total, dim = h.shape
    tokens = cos.shape[0] * SEQS
    chunks = total // tokens
    rank = bq.shape[1]
    bc = dim // n_dev
    n_chip = n_dev // 2
    width = wq.shape[1]

    def whole(a):
        nd = a.ndim
        return pl.BlockSpec(a.shape, lambda c: (0,) * nd, pipeline_mode=pl.Buffered(1))

    def later(c):
        return jnp.maximum(c - chunks, 0)

    return pl.pallas_call(
        functools.partial(attention_kernel, scale, n_dev),
        grid=(2 * chunks,),
        in_specs=[
            pl.BlockSpec(memory_space=pltpu.SMEM),
            pl.BlockSpec((tokens, dim), lambda c: (jnp.minimum(jnp.where(c < chunks - 1, c, c - 1), chunks - 1), 0)),
            ANY,
            ANY,
            whole(wq), whole(wk), whole(wv), whole(bq), whole(bk), whole(bv), whole(wo), whole(ao), whole(bo), whole(cos), whole(sin),
        ],
        out_specs=[
            pl.BlockSpec((1, 2, n_chip, tokens, bc), lambda c: (later(c),) + (0,) * 4),
            pl.BlockSpec((1, 2, n_chip, tokens // n_dev, rank), lambda c: (later(c),) + (0,) * 4),
            ANY,
        ],
        scratch_shapes=[
            pltpu.VMEM((chunks, 3, tokens, width), F32),
            pltpu.VMEM((3, tokens, rank), BF16),
            pltpu.VMEM((tokens, width), BF16),
            pltpu.VMEM((2, n_chip) + low.shape, BF16),
            pltpu.VMEM((tokens, bc), BF16),
            *exchange_bufs(n_chip, tokens, bc),
            *exchange_bufs(n_chip, tokens // n_dev, rank),
            pltpu.SemaphoreType.DMA((3,)),
            pltpu.SemaphoreType.DMA((5, 10)),
            pltpu.SemaphoreType.DMA((5, 10)),
        ],
        out_shape=[
            jax.ShapeDtypeStruct((chunks, 2, n_chip, tokens, bc), BF16),
            jax.ShapeDtypeStruct((chunks, 2, n_chip, tokens // n_dev, rank), BF16),
            jax.ShapeDtypeStruct((2, n_chip, tokens, bc), BF16),
        ],
        compiler_params=pltpu.CompilerParams(collective_id=1, has_side_effects=True, vmem_limit_bytes=67043328),
        cost_estimate=pl.CostEstimate(flops=2 * total * dim * width * 4, bytes_accessed=6 * total * dim, transcendentals=0),
        name="attention_stage",
    )(ids, h, low, x, wq, wk, wv, bq, bk, bv, wo, ao, bo, cos, sin)


LEAD = 5
TAIL = 10
NEVER = -100
FIRST = (NEVER,) * 9 + (-5, -3, -2, -1)
SECOND = (-5, -1, *range(2, 7), 10, 12, 13, *range(15, 18))
LATER = (7, 11, *range(16, 21), 24, 27, 28, 31, 33, 35)
R1_PLAN = ((0, FIRST), (0, SECOND), (0, LATER), (1, LATER))
DOWN_NEXT = (3, 8, 12, *range(14, 18), 20, 22, 24)
DOWN_THEN = (0, 3, *range(7, 12), 14, 16, 17)
R2_PLAN = ((1, DOWN_NEXT), (2, DOWN_NEXT), (3, DOWN_THEN), (4, tuple(range(TAIL))))


def window_of(tick, per):
    later = jnp.maximum(tick - LEAD, 0)
    return jnp.where(tick < LEAD, 0, 1 + later // per), jnp.where(tick < LEAD, tick, lax.rem(later, per))


def mlp_kernel(scale, n_dev, ids_ref, part_hbm, lowo_hbm, x_hbm, g0_hbm, bo_hbm, bd_hbm, agate_hbm, aup_hbm, gain_ref,
               wg_ref, wu_ref, bg_ref, bu_ref, ad_ref, wd_ref, y_hbm,
               h2, lowg, lowu, m_ref, lowd, x1own, xres, bo, bd, agu,
               q1, d1, ra1, rb1, ol1, or1, g1, lq1, ld1, lra1, lrb1, lol1, lor1, lg1, gu,
               part2, q2, d2, ra2, rb2, ol2, or2, g2, lpart2, lq2, ld2, lra2, lrb2, lol2, lor2, lg2,
               load_sem, own_sem, y_sem, s_sem, r_sem):
    tick = pl.program_id(0)
    me = lax.axis_index("tensor")
    place = placement(n_dev)
    k, i, n = place[:3]
    chunks, _, _, tokens, bc = part_hbm.shape
    seq = tokens // SEQS
    gate_ticks = m_ref.shape[1] // TILE_N
    dim = h2.shape[2]
    per_w = gate_ticks + dim // TILE_D
    w, j = window_of(tick, per_w)

    def sems(t):
        return [ref.at[t, part] for part in range(2) for ref in (s_sem, r_sem)]

    e1 = Exchange(place, d1, q1, ra1, rb1, ol1, or1, g1, *sems(0))
    f1 = Exchange(place, ld1, lq1, lra1, lrb1, lol1, lor1, lg1, *sems(1))
    e2 = Exchange(place, d2, q2, ra2, rb2, ol2, or2, g2, *sems(2))
    f2 = Exchange(place, ld2, lq2, lra2, lrb2, lol2, lor2, lg2, *sems(3))
    eg = gather_only(place, gu, *sems(4)[2:])

    half_gu = agu.shape[1] // 2

    def loads():
        return [pltpu.make_async_copy(src, dst, load_sem.at[t])
                for t, (src, dst) in enumerate(((g0_hbm, g1), (agate_hbm, agu.at[:, :half_gu]), (aup_hbm, agu.at[:, half_gu:]), (g0_hbm.at[k, i], x1own.at[0]), (bo_hbm, bo), (bd_hbm, bd)))]

    def rows_of(s):
        return pl.ds(s * seq, seq)

    @pl.when(tick == 0)
    def _():
        barrier = greet(place)
        for cp in loads():
            cp.start()
        pl.semaphore_wait(barrier, 3)

    def own_loads(c):
        return (
            pltpu.make_async_copy(part_hbm.at[c, k], q1, own_sem.at[0]),
            pltpu.make_async_copy(lowo_hbm.at[c, k], lq1, own_sem.at[1]),
            pltpu.make_async_copy(x_hbm.at[pl.ds(c * tokens, tokens), pl.ds(pl.multiple_of(me * bc, bc), bc)], xres, own_sem.at[2]),
        )

    def p1_0(c):
        f1.rs_copy(0, lowo_hbm.at[c, 1 - k]).start()
        e1.rs_copy(0, part_hbm.at[c, 1 - k]).start()
        for cp in own_loads(c):
            cp.start()

    def p1_1(c):
        for cp in own_loads(c):
            cp.wait()
        f1.start_rs(lq1)
        e1.start_rs(q1)
        f1.rs_copy(0, lowo_hbm.at[c, 1 - k]).wait_send()
        e1.rs_copy(0, part_hbm.at[c, 1 - k]).wait_send()

    def p1_2(c):
        f1.relay_rs()
        e1.relay_rs()

    def final_sum(e, f, resid, table, chunk, keep):
        total_block(scale, e, f, resid, table, ids_ref, chunk, keep)

    def p1_6(c):
        final_sum(e1, f1, xres, bo, c, x1own.at[c])

    def p1_9(c):
        @pl.when(c == 0)
        def _():
            for cp in loads():
                cp.wait()

        pl.when(c > 0)(e1.end_ag)
        hc = h2.at[lax.rem(c, 2)]
        slab = 32

        def body(t, carry):
            r = pl.ds(pl.multiple_of(t * slab, slab), slab)
            tot = None
            for b in range(n_dev):
                v = g1[b % 2, b // 2, r, :].astype(F32)
                tot = v * v if tot is None else tot + v * v
            inv = lax.rsqrt(jnp.sum(tot, axis=-1, keepdims=True) / dim + EPSILON)
            for b in range(n_dev):
                v = g1[b % 2, b // 2, r, :].astype(F32)
                hc[r, bc * b:bc * (b + 1)] = (v * inv * gain_ref[:, bc * b:bc * (b + 1)]).astype(BF16)
            return carry

        lax.fori_loop(0, tokens // slab, body, 0)
        for s in range(SEQS):
            ident = ids_ref[c * SEQS + s]
            low = dot(hc[rows_of(s), :], agu[ident], NT)
            gu[k, i, :, s * seq:(s + 1) * seq] = jnp.transpose(low).astype(BF16)
        eg.start_ag()

    def p1_12(c):
        eg.end_ag()
        slot = lax.rem(c, 2)
        half = gu.shape[2] // 2
        for p, ref in enumerate((lowg, lowu)):
            cat = jnp.concatenate([gu[d % 2, d // 2, half * p:half * (p + 1), :] for d in range(n_dev)])
            ref[slot] = jnp.transpose(cat.astype(F32)).astype(BF16)

    steps1 = (p1_0, p1_1, p1_2, lambda c: low_sum(f1), lambda c: f1.relay_ag(), lambda c: f1.last_ag(), p1_6,
              lambda c: e1.relay_ag(), lambda c: e1.last_ag(), p1_9, lambda c: eg.relay_ag(), lambda c: eg.last_ag(), p1_12)

    def y_copies(c):
        rows = pl.ds(c * tokens, tokens)
        return [pltpu.make_async_copy(g2.at[b % 2, b // 2], y_hbm.at[rows, pl.ds(b * bc, bc)], y_sem.at[b]) for b in range(n_dev)]

    def p2_0(c):
        f2.rs_copy(0, lpart2.at[1 - k]).start()
        e2.rs_copy(0, part2.at[1 - k]).start()

    def p2_1(c):
        f2.start_rs(lpart2.at[k])
        e2.start_rs(part2.at[k])
        f2.rs_copy(0, lpart2.at[1 - k]).wait_send()
        e2.rs_copy(0, part2.at[1 - k]).wait_send()

    def p2_2(c):
        f2.relay_rs()
        e2.relay_rs()

    def p2_6(c):
        final_sum(e2, f2, x1own.at[c], bd, c, None)

    def p2_9(c):
        e2.end_ag()
        for cp in y_copies(c):
            cp.start()
        for cp in y_copies(c):
            cp.wait()

    steps2 = (p2_0, p2_1, p2_2, lambda c: low_sum(f2), lambda c: f2.relay_ag(), lambda c: f2.last_ag(), p2_6,
              lambda c: e2.relay_ag(), lambda c: e2.last_ag(), p2_9)

    def place_steps(plan, steps):
        for t, step in enumerate(steps):
            marks = [LEAD + start * per_w + ticks[t] for start, ticks in plan]
            hit = functools.reduce(jnp.logical_or, [tick == mark for mark in marks])

            def run(step=step, marks=marks):
                chunk = 0
                for mark in marks[1:]:
                    chunk = chunk + jnp.where(tick >= mark, 1, 0)
                step(chunk)

            pl.when(hit)(run)

    place_steps(R1_PLAN, steps1)
    place_steps(R2_PLAN, steps2)

    live = (w >= 1) & (w <= chunks)

    @pl.when(live & (j == 0))
    def _():
        lowd[...] = jnp.zeros_like(lowd)

    @pl.when(live & (j < gate_ticks))
    def _():
        slot = lax.rem(w + 1, 2)
        g = dot(h2[slot], wg_ref[...])
        u = dot(h2[slot], wu_ref[...])
        cols = pl.ds(pl.multiple_of(j * TILE_N, TILE_N), TILE_N)
        for s in range(SEQS):
            r = rows_of(s)
            ident = ids_ref[(w - 1) * SEQS + s]
            gs = g[s * seq:(s + 1) * seq] + scale * dot(lowg[slot, r, :], bg_ref[ident])
            us = u[s * seq:(s + 1) * seq] + scale * dot(lowu[slot, r, :], bu_ref[ident])
            mm = (jax.nn.silu(gs) * us).astype(BF16)
            m_ref[r, cols] = mm
            lowd[r, :] += dot(mm, ad_ref[ident])

    @pl.when(live & (j == gate_ticks))
    def _():
        rows = lpart2.shape[2]
        for b in range(n_dev):
            lpart2[b // n, b % n] = lowd[b * rows:(b + 1) * rows, :].astype(BF16)

    @pl.when(live & (j >= gate_ticks))
    def _():
        jj = j - gate_ticks
        val = dot(m_ref[...], wd_ref[...]).astype(BF16)
        per = bc // 128
        for t in range(TILE_D // 128):
            unit = jj * (TILE_D // 128) + t
            b = unit // per
            off = pl.multiple_of((unit - b * per) * 128, 128)
            part2[lax.rem(b, 2), b // 2, :, pl.ds(off, 128)] = val[:, t * 128:(t + 1) * 128]


def mlp_stage(ids, part, lowo, x, g0, bo, bd, agate, aup, gain, wg, wu, bg, bu, ad, wd, scale, n_dev):
    chunks, _, n_chip, tokens, bc = part.shape
    total, dim = x.shape
    ffn = wg.shape[1]
    n_ad, rank = bo.shape[0], bo.shape[1]
    lrows = tokens // n_dev
    gur = 2 * agate.shape[1]
    gt = ffn // TILE_N
    dt = dim // TILE_D

    def gate_idx(tick):
        w, j = window_of(tick, gt + dt)
        return jnp.where(w == 0, 0, jnp.where(w > chunks, gt - 1, jnp.minimum(j, gt - 1)))

    def down_idx(tick):
        w, j = window_of(tick, gt + dt)
        return jnp.where(w == 0, 0, jnp.where(w > chunks, dt - 1, jnp.maximum(j - gt, 0)))

    bufs = functools.partial(exchange_bufs, n_chip)

    return pl.pallas_call(
        functools.partial(mlp_kernel, scale, n_dev),
        grid=(LEAD + chunks * (gt + dt) + TAIL,),
        in_specs=[
            pl.BlockSpec(memory_space=pltpu.SMEM), ANY, ANY, ANY, ANY, ANY, ANY, ANY, ANY,
            pl.BlockSpec((1, dim), lambda t: (0, 0)),
            pl.BlockSpec((dim, TILE_N), lambda t: (0, gate_idx(t))),
            pl.BlockSpec((dim, TILE_N), lambda t: (0, gate_idx(t))),
            pl.BlockSpec((n_ad, rank, TILE_N), lambda t: (0, 0, gate_idx(t))),
            pl.BlockSpec((n_ad, rank, TILE_N), lambda t: (0, 0, gate_idx(t))),
            pl.BlockSpec((n_ad, TILE_N, rank), lambda t: (0, gate_idx(t), 0)),
            pl.BlockSpec((ffn, TILE_D), lambda t: (0, down_idx(t))),
        ],
        out_specs=ANY,
        out_shape=jax.ShapeDtypeStruct((total, dim), BF16),
        scratch_shapes=[
            pltpu.VMEM((2, tokens, dim), BF16),
            pltpu.VMEM((2, tokens, rank), BF16),
            pltpu.VMEM((2, tokens, rank), BF16),
            pltpu.VMEM((tokens, ffn), BF16),
            pltpu.VMEM((tokens, rank), F32),
            pltpu.VMEM((chunks, tokens, bc), BF16),
            pltpu.VMEM((tokens, bc), BF16),
            pltpu.VMEM(bo.shape, BF16),
            pltpu.VMEM(bd.shape, BF16),
            pltpu.VMEM((n_ad, gur, dim), BF16),
            *bufs(tokens, bc),
            *bufs(lrows, rank),
            pltpu.VMEM((2, n_chip, gur, tokens), BF16),
            pltpu.VMEM((2, n_chip, tokens, bc), BF16),
            *bufs(tokens, bc),
            pltpu.VMEM((2, n_chip, lrows, rank), BF16),
            *bufs(lrows, rank),
            pltpu.SemaphoreType.DMA((6,)),
            pltpu.SemaphoreType.DMA((3,)),
            pltpu.SemaphoreType.DMA((n_dev,)),
            pltpu.SemaphoreType.DMA((5, 2, 10)),
            pltpu.SemaphoreType.DMA((5, 2, 10)),
        ],
        compiler_params=pltpu.CompilerParams(collective_id=0, has_side_effects=True, vmem_limit_bytes=67043328),
        name="mlp_stage",
    )(ids, part, lowo, x, g0, bo, bd, agate, aup, gain, wg, wu, bg, bu, ad, wd)


def solution(mesh):
    tp_size = mesh.shape['tensor']
    free = None
    second = P(free, 'tensor')
    third = P(free, free, 'tensor')
    in_specs = (P('data'), P('data'), P(), P(), *[second] * 3, P('tensor'), second, second, P('tensor'),
                *[third] * 6, second, *[third] * 5, second, third)

    def local_layer(x_in, adapter_ids, gain_attn, gain_mlp, w_q, w_k, w_v, w_o, w_gate, w_up, w_down, a_q, b_q, a_k, b_k, a_v, b_v, a_o, b_o, a_gate, b_gate, a_up, b_up, a_down, b_down):
        scale = ALPHA / b_q.shape[1]
        batch, seq, dim = x_in.shape
        head = w_q.shape[2]
        half = head // 2
        n_ad, rank = b_q.shape[:2]

        def flip(a):
            return jnp.swapaxes(a, 1, 2)

        def flat(w):
            rows = lax.optimization_barrier(w.reshape((-1,) + w.shape[-2:]))
            wide = lax.optimization_barrier(rows.reshape(rows.shape[0], -1))
            return wide.reshape(w.shape[:-2] + wide.shape[1:])

        h, low = rank_products(adapter_ids, x_in, gain_attn[None, :], flip(a_q), flip(a_k), flip(a_v))
        inv_freq = ROPE_BASE ** (-2.0 * jnp.arange(half, dtype=F32) / head)
        angle = jnp.arange(seq, dtype=F32)[:, None] * inv_freq[None, :]
        x = x_in.reshape(batch * seq, dim)
        part, lowo, g0 = attention_stage(adapter_ids, h, low, x, flat(w_q), flat(w_k), flat(w_v), flat(b_q), flat(b_k), flat(b_v),
                                         w_o.reshape(-1, dim), a_o.reshape(n_ad, -1, rank), b_o, jnp.cos(angle), jnp.sin(angle), scale, tp_size)
        y = mlp_stage(adapter_ids, part, lowo, x, g0, b_o, b_down, flip(a_gate), flip(a_up), gain_mlp[None, :],
                      w_gate, w_up, b_gate, b_up, a_down, w_down, scale, tp_size)
        return y.reshape(batch, seq, dim)

    return jax.shard_map(local_layer, mesh=mesh, in_specs=in_specs, out_specs=P('data'), check_vma=False)
```
